32 devices in a mesh: dp: 8 (over z, x), mp: 4 (over y, core).
Axes of the slice: x: 2, y: 2, z: 4, core: 2. Of those that a mesh axis runs over, the one named last changes fastest.
Arguments:
- gradients: bfloat16 [8, 3584, 14336], P(None, 'dp', 'mp'), may hold values from -60 to 60
- column_slot: int32 [8, 16], replicated, may hold values from 0 to 31, as said below
- left_roots: bfloat16 [32, 4, 4, 896, 896], P('dp', 'mp'), may hold values from -1 to 5
- right_roots: bfloat16 [32, 4, 4, 896, 896], P('dp', 'mp'), may hold values from -1 to 5
Outputs:
- update: bfloat16 [8, 3584, 14336], P(None, 'dp', 'mp')
- clip_scale: float32 [], replicated
The draws below stay inside these ranges and needn't reach their ends.
Inputs may be any that keep to these rules, and one draw needn't show every extreme that they name: `column_slot`: block column c belongs to group c // 4; over all matrices, the entries of one group's block columns are a permutation of 0 to 31.
All inputs are finite; a program needn't handle non-finite values.
Results may differ from the reference program's by a relative error of at most 0.0049.
Values may be sent and summed in bfloat16 or wider, within the bound.
No kernel may reach another device: no remote copies, remote signals or barrier semaphores. Data moves between devices by JAX's collectives and lax.ppermute only.
A program may use at most 256 MiB of HBM per device.

```python
import math
import jax
import jax.numpy as jnp
from jax import lax

D = 3584
FF = 14336
BLOCK = 896
MATRICES = 8
ROW_BLOCKS = 4
COLUMNS = 16
COLS_MP = 4
SLOTS = 32
N_MP = 4


def draw_gradients(key, part):
    keys = jax.random.split(jax.random.fold_in(key, 5), 3)
    ramp = jnp.sqrt(1.0 + 2.0 * jnp.arange(D, dtype=jnp.float32) / (D - 1)).reshape(1, D, 1)
    col_scale = jnp.exp(jax.random.uniform(keys[1], (MATRICES, 1, FF), jnp.float32, 0.0, math.log(10.0)))
    row_scale = jnp.exp(jax.random.uniform(keys[0], (MATRICES, D, 1), jnp.float32, 0.0, math.log(10.0)))
    base = jnp.clip(jax.random.normal(keys[2], (MATRICES, D, FF), jnp.float32), -6.0, 6.0)
    values = base * row_scale * col_scale * ramp / 21.5
    return jnp.clip(values, -60.0, 60.0).astype(jnp.bfloat16)


def draw_column_slot(key, part):
    keys = jax.random.split(jax.random.fold_in(key, 11), N_MP)

    def permute_one(sub_key):
        return jax.random.permutation(sub_key, SLOTS)
    perms = jax.vmap(permute_one)(keys).astype(jnp.int32)
    table = perms.reshape(N_MP, MATRICES, COLS_MP).transpose(1, 0, 2).reshape(MATRICES, COLUMNS)
    return table.astype(jnp.int32)


def draw_roots(key):
    keys = jax.random.split(key, 2)
    shape = (SLOTS, N_MP, ROW_BLOCKS, BLOCK, BLOCK)
    noise = jnp.clip(jax.random.normal(keys[0], shape, jnp.float32), -4.0, 4.0)
    symmetric = (noise + jnp.swapaxes(noise, -1, -2)) * (0.35 / math.sqrt(2.0 * BLOCK))
    diagonal = jnp.exp(jax.random.uniform(keys[1], shape[:-1], jnp.float32, math.log(0.5), math.log(2.0)))
    matrix = symmetric + diagonal[..., None] * jnp.eye(BLOCK, dtype=jnp.float32)
    return matrix.astype(jnp.bfloat16)


def draw_left_roots(key, part):
    return draw_roots(jax.random.fold_in(key, 21))


def draw_right_roots(key, part):
    return draw_roots(jax.random.fold_in(key, 37))


def setup_inputs(seed: int = 0) -> dict:
    splits = jax.random.split(jax.random.key(seed), 5)
    gradients = draw_gradients(jax.random.fold_in(splits[4], 71), 0)
    column_slot = draw_column_slot(jax.random.fold_in(splits[4], 71), 0)
    left_roots = draw_left_roots(jax.random.fold_in(splits[4], 71), 0)
    right_roots = draw_right_roots(jax.random.fold_in(splits[4], 71), 0)
    return {"gradients": gradients, "column_slot": column_slot, "left_roots": left_roots, "right_roots": right_roots}


rms_limit = 0.25
epsilon = 1e-06

def reference(gradients, column_slot, left_roots, right_roots):
    widened = gradients.astype(jnp.float32)
    square_sum = jnp.sum(widened * widened)
    mean_square = square_sum / (MATRICES * D * FF)
    clip_scale = jnp.minimum(jnp.float32(1.0), rms_limit / jnp.sqrt(mean_square + epsilon)).astype(jnp.float32)
    zero_index = jnp.zeros((), jnp.int32)

    def one_column(flat_index):
        matrix = (flat_index // COLUMNS).astype(jnp.int32)
        block_col = (flat_index % COLUMNS).astype(jnp.int32)
        group_index = (block_col // COLS_MP).astype(jnp.int32)
        slot_index = column_slot[matrix, block_col].astype(jnp.int32)
        block_grad = lax.dynamic_slice(gradients, (matrix, zero_index, (block_col * BLOCK).astype(jnp.int32)), (1, D, BLOCK))
        block_grad = block_grad.reshape(ROW_BLOCKS, BLOCK, BLOCK).astype(jnp.float32)
        starts = (slot_index, group_index, zero_index, zero_index, zero_index)
        left_root = lax.dynamic_slice(left_roots, starts, (1, 1, ROW_BLOCKS, BLOCK, BLOCK)).reshape(ROW_BLOCKS, BLOCK, BLOCK)
        right_root = lax.dynamic_slice(right_roots, starts, (1, 1, ROW_BLOCKS, BLOCK, BLOCK)).reshape(ROW_BLOCKS, BLOCK, BLOCK)
        first_product = jnp.einsum('nab,nbc->nac', left_root.astype(jnp.float32), block_grad)
        scaled = (clip_scale * first_product).astype(jnp.bfloat16)
        second_product = jnp.einsum('nab,nbc->nac', scaled.astype(jnp.float32), right_root.astype(jnp.float32))
        return second_product.astype(jnp.bfloat16).reshape(D, BLOCK)
    columns = lax.map(one_column, jnp.arange(MATRICES * COLUMNS, dtype=jnp.int32))
    update = columns.reshape(MATRICES, COLUMNS, D, BLOCK).transpose(0, 2, 1, 3).reshape(MATRICES, D, FF)
    return (update, clip_scale)
```

```python
import functools

import jax
import jax.numpy as jnp
from jax import lax
from jax.experimental import pallas as pl
from jax.experimental.pallas import tpu as pltpu
from jax.sharding import PartitionSpec as P

rms_limit = 0.25
epsilon = 1e-06
in_flight = 8


HBM = pl.BlockSpec(memory_space=pl.ANY)
SMEM = pl.BlockSpec(memory_space=pltpu.SMEM)


def place(ref, position, local_cols, block):
    matrix = lax.div(position, local_cols)
    start = pl.multiple_of(lax.rem(position, local_cols) * block, 128)
    return ref.at[matrix, :, pl.ds(start, block)]


def gather_kernel(first, count, local_cols, block, position, gradients, *refs):
    pieces, (held, in_sem, out_sem) = refs[:count], refs[count:]
    loads = [
        pltpu.make_async_copy(
            place(gradients, position[first + k], local_cols, block), held.at[k], in_sem.at[k]
        )
        for k in range(count)
    ]
    stores = [
        pltpu.make_async_copy(held.at[k], pieces[k], out_sem.at[k]) for k in range(count)
    ]
    for load in loads:
        load.start()
    for load, store in zip(loads, stores):
        load.wait()
        store.start()
    for store in stores:
        store.wait()


def gather(position, gradients, first, count, block):
    _, rows, width = gradients.shape
    return pl.pallas_call(
        functools.partial(gather_kernel, first, count, width // block, block),
        out_shape=[jax.ShapeDtypeStruct((rows, block), gradients.dtype)] * count,
        in_specs=[SMEM, HBM],
        out_specs=[HBM] * count,
        scratch_shapes=[
            pltpu.VMEM((count, rows, block), gradients.dtype),
            pltpu.SemaphoreType.DMA((count,)),
            pltpu.SemaphoreType.DMA((count,)),
        ],
        cost_estimate=pl.CostEstimate(
            flops=count * rows * block * 512, bytes_accessed=count * rows * block * 4, transcendentals=0
        ),
        name="gather",
    )(position, gradients)


def scatter_kernel(first, count, local_cols, block, position, *refs):
    pieces = refs[:count]
    out, held, in_sem, out_sem = refs[-4:]
    loads = [
        pltpu.make_async_copy(pieces[k], held.at[k], in_sem.at[k]) for k in range(count)
    ]
    stores = [
        pltpu.make_async_copy(
            held.at[k], place(out, position[first + k], local_cols, block), out_sem.at[k]
        )
        for k in range(count)
    ]
    for load in loads:
        load.start()
    for load, store in zip(loads, stores):
        load.wait()
        store.start()
    for store in stores:
        store.wait()


def scatter(position, pieces, out, shape, first, block):
    count = len(pieces)
    rows = shape[1]
    operands = [position, *pieces] + ([] if out is None else [out])
    return pl.pallas_call(
        functools.partial(scatter_kernel, first, count, shape[2] // block, block),
        out_shape=jax.ShapeDtypeStruct(shape, pieces[0].dtype),
        in_specs=[SMEM] + [HBM] * (len(operands) - 1),
        out_specs=HBM,
        scratch_shapes=[
            pltpu.VMEM((count, rows, block), pieces[0].dtype),
            pltpu.SemaphoreType.DMA((count,)),
            pltpu.SemaphoreType.DMA((count,)),
        ],
        input_output_aliases={} if out is None else {count + 1: 0},
        cost_estimate=pl.CostEstimate(
            flops=count * rows * block * 512, bytes_accessed=count * rows * block * 4, transcendentals=0
        ),
        name="scatter",
    )(*operands)


def precondition_kernel(parts, rows, where, clip, left, right, *refs):
    pieces, outs, (held, sem) = refs[:parts], refs[parts : 2 * parts], refs[2 * parts :]
    part, tile = pl.program_id(0), pl.program_id(1)

    @pl.when((part == 0) & (tile == 0))
    def _():
        loads = [
            pltpu.make_async_copy(
                pieces[b],
                held.at[pl.ds(pl.multiple_of(where[1 + b] * rows, 16), rows)],
                sem.at[b],
            )
            for b in range(parts)
        ]
        for load in loads:
            load.start()
        for load in loads:
            load.wait()

    first = jnp.dot(left[0, 0, 0], held[...], preferred_element_type=jnp.float32)
    scaled = (clip[0] * first).astype(held.dtype)
    second = jnp.dot(scaled, right[0, 0, 0], preferred_element_type=jnp.float32)
    finished = second.astype(held.dtype)
    for b in range(parts):

        @pl.when(part == b)
        def _():
            outs[b][...] = finished


def precondition(where, clip, left_roots, right_roots, pieces, slot):
    parts = len(pieces)
    rows, block = pieces[0].shape
    height = max(t for t in range(16, 257, 16) if rows % t == 0)
    tiles = rows // height

    def out_index(b):
        def index(part, tile, *_):
            return (jnp.where(part == b, tile, jnp.where(part < b, 0, tiles - 1)), 0)

        return index

    return pl.pallas_call(
        functools.partial(precondition_kernel, parts, rows),
        grid_spec=pltpu.PrefetchScalarGridSpec(
            num_scalar_prefetch=2,
            grid=(parts, tiles),
            in_specs=[
                pl.BlockSpec(
                    (1, 1, 1, height, block),
                    lambda part, tile, where, clip: (slot, 0, where[0], where[1 + part] * tiles + tile, 0),
                ),
                pl.BlockSpec(
                    (1, 1, 1, block, block),
                    lambda part, tile, where, clip: (slot, 0, where[0], 0, 0),
                ),
            ]
            + [HBM] * parts,
            out_specs=[pl.BlockSpec((height, block), out_index(b)) for b in range(parts)],
            scratch_shapes=[
                pltpu.VMEM((block, block), pieces[0].dtype),
                pltpu.SemaphoreType.DMA((parts,)),
            ],
        ),
        out_shape=[jax.ShapeDtypeStruct((rows, block), pieces[0].dtype)] * parts,
        cost_estimate=pl.CostEstimate(
            flops=4 * block**3, bytes_accessed=8 * block**2, transcendentals=0
        ),
        name="precondition",
    )(where, clip, left_roots, right_roots, *pieces)


def body(gradients, column_slot, left_roots, right_roots):
    matrices, rows, width = gradients.shape
    rounds, _, row_blocks, block = left_roots.shape[:4]
    local_cols = width // block
    devices, groups = lax.axis_size("dp"), lax.axis_size("mp")
    parts = devices // row_blocks
    me = lax.axis_index("dp")

    my_slots = lax.dynamic_slice_in_dim(
        column_slot, lax.axis_index("mp") * local_cols, local_cols, 1
    ).reshape(-1)
    partner = jnp.arange(devices, dtype=jnp.int32) ^ me
    wanted = partner[None, :] * rounds + jnp.arange(rounds, dtype=jnp.int32)[:, None]
    places = jnp.arange(matrices * local_cols, dtype=jnp.int32)
    position = jnp.sum(
        jnp.where(my_slots == wanted[..., None], places, 0), axis=-1, dtype=jnp.int32
    ).reshape(-1)
    heights = [
        jnp.stack([(me // parts) ^ a] + [(me % parts) ^ b for b in range(parts)]).astype(jnp.int32)
        for a in range(row_blocks)
    ]

    far, near = list(range(devices // 2, devices)), list(range(1, devices // 2))
    mixed = [k for pair in zip(far, near) for k in pair] + far[len(near) :]
    sent = []

    def send(piece, k):
        if len(sent) >= in_flight:
            piece, _ = lax.optimization_barrier((piece, sent[-in_flight]))
        sent.append(lax.ppermute(piece, "dp", [(d, d ^ k) for d in range(devices)]))
        return sent[-1]

    arrived = []
    for j in range(rounds):
        pieces = gather(position, gradients, j * devices, devices, block)
        if j == 0:
            opened, _ = lax.optimization_barrier((gradients, pieces[0]))
        got = {k: send(pieces[k], k) for k in mixed}
        got[0] = pieces[0]
        arrived.append(got)

    share = lax.psum(jnp.sum(jnp.square(opened.astype(jnp.float32))), "mp")
    share = jnp.broadcast_to(share, (8, 128))
    sums = [share] + [
        lax.ppermute(share, "dp", [(d, d ^ k) for d in range(devices)]) for k in range(1, devices)
    ]
    sums, _ = lax.optimization_barrier((sums, arrived[0][mixed[-1]]))
    while len(sums) > 1:
        sums = [a + b for a, b in zip(sums[::2], sums[1::2])]
    square_sum = sums[0][0, 0]
    total = gradients.size * devices * groups
    clip_scale = jnp.minimum(
        jnp.float32(1.0), rms_limit / jnp.sqrt(square_sum / total + epsilon)
    )

    update = None
    returned = []
    for j in range(rounds):
        got = arrived[j]
        done = {}
        for a in range(row_blocks):
            pieces = [got[a * parts + b] for b in range(parts)]
            outs = precondition(
                heights[a], clip_scale.reshape(1), left_roots, right_roots, pieces, j
            )
            for b in range(parts):
                done[a * parts + b] = outs[b]
        order = mixed if j + 1 < rounds else near + far
        back = {k: send(done[k], k) for k in order}
        back[0] = done[0]
        returned.append(back)
    for j in range(rounds):
        for a in range(row_blocks):
            first = a * parts
            pieces = [returned[j][first + b] for b in range(parts)]
            update = scatter(position, pieces, update, gradients.shape, j * devices + first, block)
    return (update, clip_scale)


def solution(mesh):
    return jax.shard_map(
        body,
        mesh=mesh,
        in_specs=(
            P(None, "dp", "mp"),
            P(),
            P("dp", "mp", None, None, None),
            P("dp", "mp", None, None, None),
        ),
        out_specs=(P(None, "dp", "mp"), P()),
        check_vma=False,
    )
```

```python
import functools

import jax
import jax.numpy as jnp
from jax import lax
from jax.experimental import pallas as pl
from jax.experimental.pallas import tpu as pltpu
from jax.sharding import PartitionSpec as P

rms_limit = 0.25
epsilon = 1e-06
in_flight = 12


HBM = pl.BlockSpec(memory_space=pl.ANY)
SMEM = pl.BlockSpec(memory_space=pltpu.SMEM)


def place(ref, position, local_cols, block):
    matrix = lax.div(position, local_cols)
    start = pl.multiple_of(lax.rem(position, local_cols) * block, 128)
    return ref.at[matrix, :, pl.ds(start, block)]


def gather_kernel(wanted, local_cols, block, position, gradients, *refs):
    count = len(wanted)
    pieces, (held, in_sem, out_sem) = refs[:count], refs[count:]
    loads = [
        pltpu.make_async_copy(
            place(gradients, position[w], local_cols, block), held.at[k], in_sem.at[k]
        )
        for k, w in enumerate(wanted)
    ]
    stores = [
        pltpu.make_async_copy(held.at[k], pieces[k], out_sem.at[k]) for k in range(count)
    ]
    for load in loads:
        load.start()
    for load, store in zip(loads, stores):
        load.wait()
        store.start()
    for store in stores:
        store.wait()


def gather(position, gradients, wanted, block):
    _, rows, width = gradients.shape
    count = len(wanted)
    return pl.pallas_call(
        functools.partial(gather_kernel, wanted, width // block, block),
        out_shape=[jax.ShapeDtypeStruct((rows, block), gradients.dtype)] * count,
        in_specs=[SMEM, HBM],
        out_specs=[HBM] * count,
        scratch_shapes=[
            pltpu.VMEM((count, rows, block), gradients.dtype),
            pltpu.SemaphoreType.DMA((count,)),
            pltpu.SemaphoreType.DMA((count,)),
        ],
        cost_estimate=pl.CostEstimate(
            flops=count * rows * block * 512, bytes_accessed=count * rows * block * 4, transcendentals=0
        ),
        name="gather",
    )(position, gradients)


def scatter_kernel(first, count, local_cols, block, position, *refs):
    pieces = refs[:count]
    out, held, in_sem, out_sem = refs[-4:]
    loads = [
        pltpu.make_async_copy(pieces[k], held.at[k], in_sem.at[k]) for k in range(count)
    ]
    stores = [
        pltpu.make_async_copy(
            held.at[k], place(out, position[first + k], local_cols, block), out_sem.at[k]
        )
        for k in range(count)
    ]
    for load in loads:
        load.start()
    for load, store in zip(loads, stores):
        load.wait()
        store.start()
    for store in stores:
        store.wait()


def scatter(position, pieces, out, shape, first, block):
    count = len(pieces)
    rows = shape[1]
    operands = [position, *pieces] + ([] if out is None else [out])
    return pl.pallas_call(
        functools.partial(scatter_kernel, first, count, shape[2] // block, block),
        out_shape=jax.ShapeDtypeStruct(shape, pieces[0].dtype),
        in_specs=[SMEM] + [HBM] * (len(operands) - 1),
        out_specs=HBM,
        scratch_shapes=[
            pltpu.VMEM((count, rows, block), pieces[0].dtype),
            pltpu.SemaphoreType.DMA((count,)),
            pltpu.SemaphoreType.DMA((count,)),
        ],
        input_output_aliases={} if out is None else {count + 1: 0},
        cost_estimate=pl.CostEstimate(
            flops=count * rows * block * 512, bytes_accessed=count * rows * block * 4, transcendentals=0
        ),
        name="scatter",
    )(*operands)


def precondition_kernel(parts, rows, where, clip, left, right, *refs):
    pieces, outs, (held, sem) = refs[:parts], refs[parts : 2 * parts], refs[2 * parts :]
    part, tile = pl.program_id(0), pl.program_id(1)

    @pl.when((part == 0) & (tile == 0))
    def _():
        loads = [
            pltpu.make_async_copy(
                pieces[b],
                held.at[pl.ds(pl.multiple_of(where[1 + b] * rows, 16), rows)],
                sem.at[b],
            )
            for b in range(parts)
        ]
        for load in loads:
            load.start()
        for load in loads:
            load.wait()

    first = jnp.dot(left[0, 0, 0], held[...], preferred_element_type=jnp.float32)
    scaled = (clip[0] * first).astype(held.dtype)
    second = jnp.dot(scaled, right[0, 0, 0], preferred_element_type=jnp.float32)
    finished = second.astype(held.dtype)
    for b in range(parts):

        @pl.when(part == b)
        def _():
            outs[b][...] = finished


def precondition(where, clip, left_roots, right_roots, pieces, slot):
    parts = len(pieces)
    rows, block = pieces[0].shape
    height = max(t for t in range(16, 257, 16) if rows % t == 0)
    tiles = rows // height

    def out_index(b):
        def index(part, tile, *_):
            return (jnp.where(part == b, tile, jnp.where(part < b, 0, tiles - 1)), 0)

        return index

    return pl.pallas_call(
        functools.partial(precondition_kernel, parts, rows),
        grid_spec=pltpu.PrefetchScalarGridSpec(
            num_scalar_prefetch=2,
            grid=(parts, tiles),
            in_specs=[
                pl.BlockSpec(
                    (1, 1, 1, height, block),
                    lambda part, tile, where, clip: (slot, 0, where[0], where[1 + part] * tiles + tile, 0),
                ),
                pl.BlockSpec(
                    (1, 1, 1, block, block),
                    lambda part, tile, where, clip: (slot, 0, where[0], 0, 0),
                ),
            ]
            + [HBM] * parts,
            out_specs=[pl.BlockSpec((height, block), out_index(b)) for b in range(parts)],
            scratch_shapes=[
                pltpu.VMEM((block, block), pieces[0].dtype),
                pltpu.SemaphoreType.DMA((parts,)),
            ],
        ),
        out_shape=[jax.ShapeDtypeStruct((rows, block), pieces[0].dtype)] * parts,
        cost_estimate=pl.CostEstimate(
            flops=4 * block**3, bytes_accessed=8 * block**2, transcendentals=0
        ),
        name="precondition",
    )(where, clip, left_roots, right_roots, *pieces)


def body(gradients, column_slot, left_roots, right_roots):
    matrices, _, width = gradients.shape
    rounds, _, row_blocks, block = left_roots.shape[:4]
    local_cols = width // block
    devices, groups = lax.axis_size("dp"), lax.axis_size("mp")
    parts = devices // row_blocks
    me = lax.axis_index("dp")

    my_slots = lax.dynamic_slice_in_dim(
        column_slot, lax.axis_index("mp") * local_cols, local_cols, 1
    ).reshape(-1)
    partner = jnp.arange(devices, dtype=jnp.int32) ^ me
    wanted = partner[None, :] * rounds + jnp.arange(rounds, dtype=jnp.int32)[:, None]
    places = jnp.arange(matrices * local_cols, dtype=jnp.int32)
    position = jnp.sum(
        jnp.where(my_slots == wanted[..., None], places, 0), axis=-1, dtype=jnp.int32
    ).reshape(-1)
    heights = [
        jnp.stack([(me // parts) ^ a] + [(me % parts) ^ b for b in range(parts)]).astype(jnp.int32)
        for a in range(row_blocks)
    ]

    far, near = list(range(devices // 2, devices)), list(range(1, devices // 2))
    mixed = [k for pair in zip(far, near) for k in pair] + far[len(near) :]
    sent = []

    def send(piece, k):
        if len(sent) >= in_flight:
            piece, _ = lax.optimization_barrier((piece, sent[-in_flight]))
        sent.append(lax.ppermute(piece, "dp", [(d, d ^ k) for d in range(devices)]))
        return sent[-1]

    arrived = []
    for j in range(rounds):
        turn = mixed[:: (-1) ** j]
        order = [*turn, 0]
        pieces = {}
        for ks in [order[:1], order[1:]] if j == 0 else [order]:
            pieces |= zip(ks, gather(position, gradients, [j * devices + k for k in ks], block))
        got = {k: send(pieces[k], k) for k in turn}
        got[0] = pieces[0]
        arrived.append(got)
        if j == 0:
            opened, _ = lax.optimization_barrier((gradients, pieces[0]))
            share = jnp.sum(jnp.square(opened.astype(jnp.float32)))
            share = lax.psum(share, "mp")
            position, share = lax.optimization_barrier((position, share))
    share = jnp.broadcast_to(share, (8, 128))
    sums = [share] + [
        lax.ppermute(share, "dp", [(d, d ^ k) for d in range(devices)]) for k in range(1, devices)
    ]
    sums, _ = lax.optimization_barrier((sums, arrived[0][mixed[-1]]))
    while len(sums) > 1:
        sums = [a + b for a, b in zip(sums[::2], sums[1::2])]
    square_sum = sums[0][0, 0]
    total = gradients.size * devices * groups
    clip_scale = jnp.minimum(
        jnp.float32(1.0), rms_limit / jnp.sqrt(square_sum / total + epsilon)
    )

    update = None
    returned = []
    for j in range(rounds):
        got = arrived[j]
        done = {}
        turn = mixed[:: (-1) ** (rounds + j)]
        for a in dict.fromkeys(k // parts for k in [*turn, 0]):
            pieces = [got[a * parts + b] for b in range(parts)]
            outs = precondition(
                heights[a], clip_scale.reshape(1), left_roots, right_roots, pieces, j
            )
            for b in range(parts):
                done[a * parts + b] = outs[b]
        back = {k: send(done[k], k) for k in turn}
        back[0] = done[0]
        returned.append(back)
    for j in range(rounds):
        for a in range(row_blocks):
            first = a * parts
            pieces = [returned[j][first + b] for b in range(parts)]
            update = scatter(position, pieces, update, gradients.shape, j * devices + first, block)
    return (update, clip_scale)


def solution(mesh):
    return jax.shard_map(
        body,
        mesh=mesh,
        in_specs=(
            P(None, "dp", "mp"),
            P(),
            P("dp", "mp", None, None, None),
            P("dp", "mp", None, None, None),
        ),
        out_specs=(P(None, "dp", "mp"), P()),
        check_vma=False,
    )
```
